128 devices in a mesh: batch: 32 (over z, y, x_hi), mp: 4 (over x_lo, core).
Axes of the slice: x: 4 (x_hi: 2, x_lo: 2; x = x_hi * 2 + x_lo), y: 4, z: 4, core: 2. Of those that a mesh axis runs over, the one named last changes fastest.
Arguments:
- lookup_ids: int32 [64, 65536], P('batch'), may hold values from 0 to 8191
- table_feature: int32 [64], replicated, may hold values from 0 to 63, each once
- tables: bfloat16 [64, 8192, 128], P('batch'), may hold values from -6 to 6
- cross_down: bfloat16 [2, 8192, 512], P(None, 'mp'), may hold values from -0.0625 to 0.0625
- cross_up: bfloat16 [2, 512, 8192], P(None, None, 'mp'), may hold values from -0.25 to 0.25
- cross_bias: float32 [2, 8192], P(None, 'mp'), may hold values from -3 to 3
Outputs:
- crossed: bfloat16 [65536, 8192], P('batch', 'mp')
The draws below stay inside these ranges and needn't reach their ends.
Inputs may be any that keep to these rules, and one draw needn't show every extreme that they name: `table_feature`: each number appears once.
All inputs are finite; a program needn't handle non-finite values.
Results may differ from the reference program's by a relative error of at most 0.015.
Values may be sent and summed in bfloat16 or wider, within the bound.
No kernel may reach another device: no remote copies, remote signals or barrier semaphores. Data moves between devices by JAX's collectives and lax.ppermute only.
A program may use at most 128 MiB of HBM per device.

```python
import math
import jax
import jax.numpy as jnp
import numpy as np
from jax import lax

FEATS = 64
EMB = 128
RANK = 512
ROWS = 8192
LAYERS = 2
WIDTH = 8192
BATCH = 65536
N_MP = 4


def plant(drawn, stream_key, low, top_value):
    place = [jax.random.randint(jax.random.fold_in(stream_key, axis), (), 0, length) for axis, length in enumerate(drawn.shape)]
    main_axis = drawn.shape.index(max(drawn.shape))
    neighbour = place[:main_axis] + [(place[main_axis] + 1) % drawn.shape[main_axis]] + place[main_axis + 1:]
    return drawn.at[tuple(place)].set(low).at[tuple(neighbour)].set(top_value)


def shard_levels(own_key, dims, pieces, low, high):
    factor_of = 1.0
    for axis_at, blocks in pieces:
        draws = jax.random.uniform(jax.random.fold_in(jax.random.fold_in(own_key, 6), axis_at), (blocks,), jnp.float32, low / len(pieces), high / len(pieces))
        factor_of = factor_of * jnp.repeat(jnp.exp(draws), dims[axis_at] // blocks).reshape((-1,) + (1,) * (len(dims) - 1 - axis_at))
    return factor_of


def rank_table(number_of, slope):
    weights = [(1 << 20) // math.isqrt(rank ** slope) + 1 for rank in range(1, number_of + 1)]
    width = 1 + sum(weights) // (1 << 30)
    return np.cumsum(np.array([max(1, weight // width) for weight in weights]))


def skewed_ids(stream_key, shape, amount, slope):
    grid = rank_table(amount, slope)
    lot = jax.random.randint(jax.random.fold_in(stream_key, 1), shape, 0, int(grid[amount - 1]))
    standing = jnp.searchsorted(jnp.asarray(grid, jnp.int32), lot, side="right")
    return jax.random.permutation(jax.random.fold_in(stream_key, 2), amount)[standing].astype(jnp.int32)


def centred(key, extent, width, bound, cuts=(), held_as=jnp.bfloat16):
    values = jax.random.normal(key, extent, jnp.float32) * width
    if len(cuts) > 0:
        values = shard_levels(key, extent, cuts, -0.22, 0.18) * values
    return jnp.clip(values, min=-bound, max=bound).astype(held_as)


def setup_inputs(seed: int = 0) -> dict:
    streams_of = jax.random.split(jax.random.key(seed), 7)
    lookup_ids = plant(skewed_ids(streams_of[0], (FEATS, BATCH), ROWS, 2), jax.random.fold_in(streams_of[0], 3), 0, ROWS - 1).astype(jnp.int32)
    table_feature = jax.random.permutation(streams_of[1], FEATS).astype(jnp.int32)
    tables = centred(streams_of[2], (FEATS, ROWS, EMB), 1.0, 6.0, ((0, 32),))
    cross_down = centred(streams_of[3], (LAYERS, WIDTH, RANK), WIDTH ** -0.5, 0.0625, ((1, 4),))
    cross_up = centred(streams_of[4], (LAYERS, RANK, WIDTH), RANK ** -0.5, 0.25, ((2, 4),))
    cross_bias = centred(streams_of[5], (LAYERS, WIDTH), 0.5, 3.0, ((1, 4),), jnp.float32)
    return dict(lookup_ids=lookup_ids, table_feature=table_feature, tables=tables, cross_down=cross_down, cross_up=cross_up, cross_bias=cross_bias)


def reference(lookup_ids, table_feature, tables, cross_down, cross_up, cross_bias):
    looked = jax.vmap(lambda table, index: jnp.take(table, index, axis=0))(tables, lookup_ids)
    inverse = jnp.zeros((FEATS,), jnp.int32).at[table_feature].set(jnp.arange(FEATS, dtype=jnp.int32))
    by_feature = jnp.take(looked, inverse, axis=0)
    embedded = jnp.transpose(by_feature, (1, 2, 0)).reshape(BATCH, EMB * FEATS)
    block = WIDTH // N_MP
    state = embedded
    for layer in range(LAYERS):
        low_sum = jnp.zeros((BATCH, RANK), jnp.float32)
        for piece in range(N_MP):
            term = jnp.dot(state[:, piece * block:(piece + 1) * block], cross_down[layer, piece * block:(piece + 1) * block, :], preferred_element_type=jnp.float32)
            rounded = lax.optimization_barrier(term.astype(jnp.bfloat16))
            low_sum = low_sum + rounded.astype(jnp.float32)
        low = low_sum.astype(jnp.bfloat16)
        high = jnp.dot(low, cross_up[layer], preferred_element_type=jnp.float32) + cross_bias[layer][None, :]
        state = (embedded.astype(jnp.float32) * high + state.astype(jnp.float32)).astype(jnp.bfloat16)
    return state
```

```python
import functools

import jax
import jax.numpy as jnp
from jax import lax
from jax.experimental import pallas as pl
from jax.experimental.pallas import tpu as pltpu
from jax.sharding import PartitionSpec as P

CHUNKS = 2
LANES = 128


def cost(flops, moved):
    return pl.CostEstimate(flops=flops, bytes_accessed=moved, transcendentals=0)


def gather_kernel(place, ids, tables, out, wide, even, odd):
    slots, rows, emb = tables.shape
    share = ids.shape[1]

    @pl.when(pl.program_id(0) == 0)
    def _():
        for slot in range(slots):
            wide[pl.ds(slot * rows, rows), :] = tables[slot].astype(jnp.float32)

    count = share // LANES
    for slot in range(slots):
        for group in range(count):
            held = even if (slot * count + group) % 2 == 0 else odd
            for row in range(LANES):
                index = ids[slot, group * LANES + row] + slot * rows
                held[pl.ds(row, 1), :] = wide[pl.ds(index, 1), :]
            turned = held[...].T.astype(jnp.bfloat16)
            out[0, :, slot, :, group * LANES : (group + 1) * LANES] = turned.reshape(
                out.shape[1], out.shape[3], LANES
            )


def looked_up(ids, tables, place, chunk, sources, groups, share):
    slots, rows, emb = tables.shape
    part = share // CHUNKS
    return pl.pallas_call(
        gather_kernel,
        grid_spec=pltpu.PrefetchScalarGridSpec(
            num_scalar_prefetch=1,
            grid=(sources,),
            in_specs=[
                pl.BlockSpec(
                    (slots, part),
                    lambda i, place: (0, (i * groups + place[0]) * CHUNKS + chunk),
                    memory_space=pltpu.SMEM,
                ),
                pl.BlockSpec((slots, rows, emb), lambda i, place: (0, 0, 0)),
            ],
            out_specs=pl.BlockSpec(
                (1, groups, slots, emb // groups, part), lambda i, place: (i, 0, 0, 0, 0)
            ),
            scratch_shapes=[
                pltpu.VMEM((slots * rows, emb), jnp.float32),
                pltpu.VMEM((LANES, emb), jnp.float32),
                pltpu.VMEM((LANES, emb), jnp.float32),
            ],
        ),
        out_shape=jax.ShapeDtypeStruct(
            (sources, groups, slots, emb // groups, part), jnp.bfloat16
        ),
        cost_estimate=cost(30_000_000_000 // CHUNKS, 12_000_000 // CHUNKS),
        name="lookup",
    )(place, ids, tables)


def first_kernel(order, moved, down, embedded, product, wide):
    feats, emb = order.shape[0], moved.shape[3]
    for feat in range(feats):
        slot = order[feat]
        wide[feat * emb : (feat + 1) * emb, :] = moved[slot // 2, 0, slot % 2].astype(jnp.float32)
    for pair in range(emb // 2):
        block = jnp.concatenate(
            [wide[pl.ds(2 * pair + k, feats, stride=emb), :] for k in range(2)], axis=0
        )
        embedded[:, pair * 2 * feats : (pair + 1) * 2 * feats] = block.T.astype(jnp.bfloat16)
    product[...] = jnp.dot(
        embedded[...], down[0], preferred_element_type=jnp.float32
    ).astype(jnp.bfloat16)


def first(moved, order, down):
    sources, groups, slots, emb, part = moved.shape
    feats = order.shape[0]
    width = feats * emb
    rank = down.shape[2]
    blocks = part // LANES
    return pl.pallas_call(
        first_kernel,
        grid_spec=pltpu.PrefetchScalarGridSpec(
            num_scalar_prefetch=1,
            grid=(groups * blocks,),
            in_specs=[
                pl.BlockSpec(
                    (sources, 1, slots, emb, LANES),
                    lambda i, order: (0, i // blocks, 0, 0, i % blocks),
                ),
                pl.BlockSpec((1, width, rank), lambda i, order: (0, 0, 0)),
            ],
            out_specs=[
                pl.BlockSpec((LANES, width), lambda i, order: (i, 0)),
                pl.BlockSpec((LANES, rank), lambda i, order: (i, 0)),
            ],
            scratch_shapes=[pltpu.VMEM((width, LANES), jnp.float32)],
        ),
        out_shape=[
            jax.ShapeDtypeStruct((groups * part, width), jnp.bfloat16),
            jax.ShapeDtypeStruct((groups * part, rank), jnp.bfloat16),
        ],
        cost_estimate=cost(2 * groups * part * width * rank, 4 * groups * part * width),
        name="first",
    )(order, moved, down)


def middle_kernel(low, embedded, up, bias, down, state, product):
    high = jnp.dot(low[...], up[0], preferred_element_type=jnp.float32) + bias[0:1, :]
    own = embedded[...].astype(jnp.float32)
    state[...] = (own * high + own).astype(jnp.bfloat16)
    product[...] = jnp.dot(
        state[...], down[0], preferred_element_type=jnp.float32
    ).astype(jnp.bfloat16)


def middle(low, embedded, up, bias, down, layer):
    rows, width = embedded.shape
    rank = low.shape[1]
    tall = min(rows, 256)
    return pl.pallas_call(
        middle_kernel,
        grid=(rows // tall,),
        in_specs=[
            pl.BlockSpec((tall, rank), lambda i: (i, 0)),
            pl.BlockSpec((tall, width), lambda i: (i, 0)),
            pl.BlockSpec((1, rank, width), lambda i: (layer, 0, 0)),
            pl.BlockSpec((1, width), lambda i: (0, 0)),
            pl.BlockSpec((1, width, rank), lambda i: (layer + 1, 0, 0)),
        ],
        out_specs=[
            pl.BlockSpec((tall, width), lambda i: (i, 0)),
            pl.BlockSpec((tall, rank), lambda i: (i, 0)),
        ],
        out_shape=[
            jax.ShapeDtypeStruct((rows, width), jnp.bfloat16),
            jax.ShapeDtypeStruct((rows, rank), jnp.bfloat16),
        ],
        cost_estimate=cost(4 * rows * width * rank, 4 * rows * width),
        name="middle",
    )(low, embedded, up, bias[layer : layer + 1], down)


def last_kernel(low, embedded, state, up, bias, *rest):
    out = rest[-1]
    high = jnp.dot(low[...], up[0], preferred_element_type=jnp.float32) + bias[0:1, :]
    out[...] = (
        embedded[...].astype(jnp.float32) * high + state[...].astype(jnp.float32)
    ).astype(jnp.bfloat16)


def last(low, embedded, state, up, bias, layer, chunk, so_far, total):
    rows, width = embedded.shape
    rank = low.shape[1]
    groups = N_GROUPS
    tall = rows // groups
    in_specs = [
        pl.BlockSpec((tall, rank), lambda i: (i, 0)),
        pl.BlockSpec((tall, width), lambda i: (i, 0)),
        pl.BlockSpec((tall, width), lambda i: (i, 0)),
        pl.BlockSpec((1, rank, width), lambda i: (layer, 0, 0)),
        pl.BlockSpec((1, width), lambda i: (0, 0)),
    ]
    args = [low, embedded, state, up, bias[layer : layer + 1]]
    aliases = {}
    if so_far is not None:
        in_specs.append(pl.BlockSpec(memory_space=pl.ANY))
        args.append(so_far)
        aliases = {5: 0}
    return pl.pallas_call(
        last_kernel,
        grid=(groups,),
        in_specs=in_specs,
        out_specs=pl.BlockSpec((tall, width), lambda i: (i * CHUNKS + chunk, 0)),
        out_shape=jax.ShapeDtypeStruct((total, width), jnp.bfloat16),
        input_output_aliases=aliases,
        cost_estimate=cost(2 * rows * width * rank, 6 * rows * width),
        name="last",
    )(*args)


N_GROUPS = 4
CORE = [(0, 1), (1, 0), (2, 3), (3, 2)]
CHIP = [(0, 2), (2, 0), (1, 3), (3, 1)]


def added(a, b):
    return (a.astype(jnp.float32) + b.astype(jnp.float32)).astype(jnp.bfloat16)


def summed(x):
    core = lax.axis_index("mp") % 2
    half = x.shape[0] // 2
    mine = lax.dynamic_slice_in_dim(x, core * half, half, 0)
    other = lax.dynamic_slice_in_dim(x, (1 - core) * half, half, 0)
    pair = added(mine, lax.ppermute(other, "mp", CORE))
    whole = added(pair, lax.ppermute(pair, "mp", CHIP))
    rest = lax.ppermute(whole, "mp", CORE)
    return jnp.concatenate(
        [jnp.where(core == 0, whole, rest), jnp.where(core == 0, rest, whole)], axis=0
    )


def per_device(lookup_ids, table_feature, tables, cross_down, cross_up, cross_bias):
    feats = table_feature.shape[0]
    sources = lax.axis_size("batch")
    groups = lax.axis_size("mp")
    total = lookup_ids.shape[1] // sources
    share = total // groups
    place = lax.axis_index("mp").reshape(1).astype(jnp.int32)
    slots = jnp.arange(feats, dtype=jnp.int32)
    order = jnp.sum(
        jnp.where(table_feature[None, :] == slots[:, None], slots[None, :], 0), axis=1
    ).astype(jnp.int32)
    out = None
    for chunk in range(CHUNKS):
        looked = looked_up(lookup_ids, tables, place, chunk, sources, groups, share)
        shape = looked.shape
        moved = lax.all_to_all(
            looked.reshape(sources * groups, *shape[2:]), ("batch", "mp"), 0, 0, tiled=True
        ).reshape(shape)
        embedded, product = first(moved, order, cross_down)
        state, product = middle(summed(product), embedded, cross_up, cross_bias, cross_down, 0)
        out = last(
            summed(product), embedded, state, cross_up, cross_bias, 1, chunk, out, total
        )
    return out


def solution(mesh):
    return jax.shard_map(
        per_device,
        mesh=mesh,
        in_specs=(
            P("batch", None),
            P(),
            P("batch", None, None),
            P(None, "mp", None),
            P(None, None, "mp"),
            P(None, "mp"),
        ),
        out_specs=P("batch", "mp"),
        check_vma=False,
    )
```

```python
import functools

import jax
import jax.numpy as jnp
from jax import lax
from jax.experimental import pallas as pl
from jax.experimental.pallas import tpu as pltpu
from jax.sharding import PartitionSpec as P


LANES = 128
SUBLANES = 8
PIECES = (2, 2)
VMEM = 60 << 20
CORE = [(0, 1), (1, 0), (2, 3), (3, 2)]
CHIP = [(0, 2), (2, 0), (1, 3), (3, 1)]
F32 = jnp.float32
BF16 = jnp.bfloat16


def cost(flops, moved):
    return pl.CostEstimate(flops=flops, bytes_accessed=moved, transcendentals=0)


def lookup_kernel(layout, place, ids, tables, out, wide, evens, odds, id_evens, id_odds, sems):
    share, stride, offset, part = layout
    slots, rows, _ = tables.shape
    step = pl.program_id(0)
    steps = pl.num_programs(0)

    def fetch(destination, which):
        start = destination * stride + place[0] * share + offset
        return pltpu.make_async_copy(
            ids.at[:, pl.ds(pl.multiple_of(start, LANES), part)],
            (id_evens, id_odds)[which],
            sems.at[which],
        )

    @pl.when(step == 0)
    def _():
        fetch(0, 0).start()
        fetch(1, 1).start()
        for slot in range(slots):
            wide[pl.ds(slot * rows, rows), :] = tables[slot].astype(F32)

    for which in range(2):
        known = (id_evens, id_odds)[which]
        fetch(2 * step + which, which).wait()
        for slot in range(slots):
            for group in range(part // LANES):
                held = (evens, odds)[(slot * (part // LANES) + group) % 2]
                for row in range(LANES):
                    index = known[slot, group * LANES + row] + slot * rows
                    held[pl.ds(row, 1), :] = wide[pl.ds(index, 1), :]
                turned = held[...].T.astype(BF16)
                out[which, :, slot, :, group * LANES : (group + 1) * LANES] = turned.reshape(
                    out.shape[1], out.shape[3], LANES
                )

        @pl.when(step + 1 < steps)
        def _():
            fetch(2 * step + 2 + which, which).start()


def looked_up(ids, tables, place, sources, groups, share, offset, part):
    slots, rows, emb = tables.shape
    count = sources * slots * part
    return pl.pallas_call(
        functools.partial(lookup_kernel, (share, groups * share, offset, part)),
        grid_spec=pltpu.PrefetchScalarGridSpec(
            num_scalar_prefetch=1,
            grid=(sources // 2,),
            in_specs=[
                pl.BlockSpec(memory_space=pltpu.HBM),
                pl.BlockSpec((slots, rows, emb), lambda i, place: (0, 0, 0)),
            ],
            out_specs=pl.BlockSpec(
                (2, groups, slots, emb // groups, part), lambda i, place: (i, 0, 0, 0, 0)
            ),
            scratch_shapes=[
                pltpu.VMEM((slots * rows, emb), F32),
                pltpu.VMEM((LANES, emb), F32),
                pltpu.VMEM((LANES, emb), F32),
                pltpu.SMEM((slots, part), jnp.int32),
                pltpu.SMEM((slots, part), jnp.int32),
                pltpu.SemaphoreType.DMA((2,)),
            ],
        ),
        out_shape=jax.ShapeDtypeStruct((sources, groups, slots, emb // groups, part), BF16),
        cost_estimate=cost(count * 1_000_000, count * emb * 2),
        compiler_params=pltpu.CompilerParams(vmem_limit_bytes=VMEM),
        name="lookup",
    )(place, ids, tables)


def first_kernel(moved, placing, down, embedded, product, turned):
    _, many, _, emb, part = moved.shape
    wide = placing.shape[1]
    for inner in range(emb // SUBLANES):
        for group in range(many):
            for piece in range(part // LANES):
                block = moved[
                    :,
                    group,
                    :,
                    inner * SUBLANES : (inner + 1) * SUBLANES,
                    piece * LANES : (piece + 1) * LANES,
                ]
                at = (group * (part // LANES) + piece) * LANES
                turned[at : at + LANES, :] = (
                    block.astype(F32).reshape(wide, LANES).T.astype(BF16)
                )
        embedded[:, inner * wide : (inner + 1) * wide] = jnp.dot(
            turned[...], placing[...], preferred_element_type=F32
        ).astype(BF16)
    product[...] = jnp.dot(embedded[...], down[0], preferred_element_type=F32).astype(BF16)


def first(moved, placing, down, rows_each):
    sources, groups, slots, emb, part = moved.shape
    wide = placing.shape[0]
    width = sources * slots * emb
    rank = down.shape[2]
    rows = groups * part
    many = rows_each // part
    return pl.pallas_call(
        first_kernel,
        grid=(groups // many,),
        in_specs=[
            pl.BlockSpec((sources, many, slots, emb, part), lambda i: (0, i, 0, 0, 0)),
            pl.BlockSpec((wide, wide), lambda i: (0, 0)),
            pl.BlockSpec((1, width, rank), lambda i: (0, 0, 0)),
        ],
        out_specs=[
            pl.BlockSpec((rows_each, width), lambda i: (i, 0)),
            pl.BlockSpec((rows_each, rank), lambda i: (i, 0)),
        ],
        scratch_shapes=[pltpu.VMEM((rows_each, wide), BF16)],
        out_shape=[
            jax.ShapeDtypeStruct((rows, width), BF16),
            jax.ShapeDtypeStruct((rows, rank), BF16),
        ],
        cost_estimate=cost(4 * rows * width * rank, 4 * rows * width),
        compiler_params=pltpu.CompilerParams(vmem_limit_bytes=VMEM),
        name="first",
    )(moved, placing, down)


def low_of(place, mine, near, far, across):
    own = pl.program_id(0) == place[0] % 2
    pair = (mine[...].astype(F32) + near[...].astype(F32)).astype(BF16).astype(F32)
    other = jnp.where(own, far[...].astype(F32), across[...].astype(F32))
    return (pair + other).astype(BF16)


def middle_kernel(place, mine, near, far, across, embedded, up, bias, down, state, product):
    low = low_of(place, mine, near, far, across)
    width = embedded.shape[1]
    tile = 512
    for at in range(0, width, tile):
        cut = slice(at, at + tile)
        high = jnp.dot(low, up[0, :, cut], preferred_element_type=F32) + bias[0:1, cut]
        own = embedded[:, cut].astype(F32)
        state[:, cut] = (own * high + own).astype(BF16)
    product[...] = jnp.dot(state[...], down[0], preferred_element_type=F32).astype(BF16)


def low_specs(half, rank):
    return [
        pl.BlockSpec((half, rank), lambda i, place: (i, 0)),
        pl.BlockSpec((half, rank), lambda i, place: (i, 0)),
        pl.BlockSpec((half, rank), lambda i, place: (0, 0)),
        pl.BlockSpec((half, rank), lambda i, place: (0, 0)),
    ]


def middle(place, lows, embedded, up, bias, down, layer):
    rows, width = embedded.shape
    rank = up.shape[1]
    half = rows // 2
    return pl.pallas_call(
        middle_kernel,
        grid_spec=pltpu.PrefetchScalarGridSpec(
            num_scalar_prefetch=1,
            grid=(2,),
            in_specs=low_specs(half, rank)
            + [
                pl.BlockSpec((half, width), lambda i, place: (i, 0)),
                pl.BlockSpec((1, rank, width), lambda i, place: (layer, 0, 0)),
                pl.BlockSpec((1, width), lambda i, place: (0, 0)),
                pl.BlockSpec((1, width, rank), lambda i, place: (layer + 1, 0, 0)),
            ],
            out_specs=[
                pl.BlockSpec((half, width), lambda i, place: (i, 0)),
                pl.BlockSpec((half, rank), lambda i, place: (i, 0)),
            ],
        ),
        out_shape=[
            jax.ShapeDtypeStruct((rows, width), BF16),
            jax.ShapeDtypeStruct((rows, rank), BF16),
        ],
        cost_estimate=cost(4 * rows * width * rank, 4 * rows * width),
        compiler_params=pltpu.CompilerParams(vmem_limit_bytes=VMEM),
        name="middle",
    )(place, *lows, embedded, up, bias, down)


def last_kernel(place, mine, near, far, across, embedded, state, up, bias, *rest):
    out = rest[-1]
    low = low_of(place, mine, near, far, across)
    width = embedded.shape[1]
    groups, part = out.shape[0], out.shape[2]
    tile = 512
    for at in range(0, width, tile):
        cut = slice(at, at + tile)
        high = jnp.dot(low, up[0, :, cut], preferred_element_type=F32) + bias[0:1, cut]
        new = (
            embedded[:, cut].astype(F32) * high + state[:, cut].astype(F32)
        ).astype(BF16)
        out[:, 0, :, cut] = new.reshape(groups, part, tile)


def last(place, lows, embedded, state, up, bias, layer, so_far, groups, offset, part, share):
    rows, width = embedded.shape
    rank = up.shape[1]
    half = rows // 2
    in_specs = low_specs(half, rank) + [
        pl.BlockSpec((half, width), lambda i, place: (i, 0)),
        pl.BlockSpec((half, width), lambda i, place: (i, 0)),
        pl.BlockSpec((1, rank, width), lambda i, place: (layer, 0, 0)),
        pl.BlockSpec((1, width), lambda i, place: (0, 0)),
    ]
    args = [place, *lows, embedded, state, up, bias]
    aliases = {}
    if so_far is not None:
        in_specs.append(pl.BlockSpec(memory_space=pltpu.HBM))
        args.append(so_far)
        aliases = {9: 0}
    return pl.pallas_call(
        last_kernel,
        grid_spec=pltpu.PrefetchScalarGridSpec(
            num_scalar_prefetch=1,
            grid=(2,),
            in_specs=in_specs,
            out_specs=pl.BlockSpec(
                (groups // 2, 1, part, width), lambda i, place: (i, 0, offset // part, 0)
            ),
        ),
        out_shape=jax.ShapeDtypeStruct((groups, 1, share, width), BF16),
        input_output_aliases=aliases,
        cost_estimate=cost(2 * rows * width * rank, 6 * rows * width),
        compiler_params=pltpu.CompilerParams(vmem_limit_bytes=VMEM),
        name="last",
    )(*args)


def summed(product):
    half = product.shape[0] // 2
    start = lax.rem(lax.axis_index("mp"), 2) * half
    near = lax.ppermute(product, "mp", CORE)
    pair = (
        lax.dynamic_slice_in_dim(product, start, half, 0).astype(F32)
        + lax.dynamic_slice_in_dim(near, start, half, 0).astype(F32)
    ).astype(BF16)
    far = lax.ppermute(pair, "mp", CHIP)
    across = lax.ppermute(far, "mp", CORE)
    return product, near, far, across


def per_device(lookup_ids, table_feature, tables, cross_down, cross_up, cross_bias):
    feats = table_feature.shape[0]
    sources = lax.axis_size("batch")
    groups = lax.axis_size("mp")
    total = lookup_ids.shape[1] // sources
    share = total // groups
    place = lax.axis_index("mp").reshape(1).astype(jnp.int32)
    same = table_feature[:, None] == jnp.arange(feats, dtype=jnp.int32)[None, :]
    row = jnp.arange(SUBLANES, dtype=jnp.int32)
    placing = (
        (same[:, None, None, :] & (row[:, None] == row[None, :])[None, :, :, None])
        .astype(BF16)
        .reshape(feats * SUBLANES, SUBLANES * feats)
    )
    out = None
    unit = share // sum(PIECES)
    parts = [piece * unit for piece in PIECES]
    offset = 0
    for part in parts:
        looked = looked_up(
            lookup_ids, tables, place, sources, groups, share, offset, part
        )
        shape = looked.shape
        moved = lax.all_to_all(
            looked.reshape(sources * groups, *shape[2:]),
            ("batch", "mp"),
            0,
            0,
            tiled=True,
        ).reshape(shape)
        embedded, product = first(moved, placing, cross_down, groups * part // 2)
        lows = summed(product)
        state, product = middle(place, lows, embedded, cross_up, cross_bias[:1], cross_down, 0)
        lows = summed(product)
        out = last(
            place,
            lows,
            embedded,
            state,
            cross_up,
            cross_bias[1:],
            1,
            out,
            groups,
            offset,
            part,
            share,
        )
        offset += part
    return out.reshape(total, -1)


def solution(mesh):
    return jax.shard_map(
        per_device,
        mesh=mesh,
        in_specs=(
            P("batch", None),
            P(),
            P("batch", None, None),
            P(None, "mp", None),
            P(None, None, "mp"),
            P(None, "mp"),
        ),
        out_specs=P("batch", "mp"),
        check_vma=False,
    )
```

```python
import functools

import jax
import jax.numpy as jnp
from jax import lax
from jax.experimental import pallas as pl
from jax.experimental.pallas import tpu as pltpu
from jax.sharding import PartitionSpec as P


LANES = 128
SUBLANES = 8
PIECES = (2, 2)
VMEM = 60 << 20
CROSS_VMEM = 24 << 20
CORE = [(0, 1), (1, 0), (2, 3), (3, 2)]
CHIP = [(0, 2), (2, 0), (1, 3), (3, 1)]
F32 = jnp.float32
BF16 = jnp.bfloat16


def cost(flops, moved):
    return pl.CostEstimate(flops=flops, bytes_accessed=moved, transcendentals=0)


def lookup_kernel(layout, place, ids, tables, out, wide, evens, odds, staged, *rest):
    share, stride, offset, part, width, sources = layout
    known, sems, moved = rest[:2], rest[2], rest[3]
    slots, rows, _ = tables.shape
    step = pl.program_id(0)
    steps = pl.num_programs(0)
    run = width // 2 * part

    def stage(destination):
        start = destination * stride + place[0] * share + offset
        return pltpu.make_async_copy(
            ids.at[:, pl.ds(pl.multiple_of(start, LANES), part)],
            staged.at[:, pl.ds(destination * part, part)],
            sems.at[destination],
        )

    def fetch(at, which):
        start = (2 * at + which) * run
        return pltpu.make_async_copy(
            staged.at[:, pl.ds(pl.multiple_of(start, LANES), run)], known[which], moved.at[which]
        )

    @pl.when(step == 0)
    def _():
        for destination in range(sources):
            stage(destination).start()
        for slot in range(slots):
            wide[pl.ds(slot * rows, rows), :] = tables[slot].astype(F32)
        for destination in range(sources):
            stage(destination).wait()
        for which in range(2):
            fetch(0, which).start()

    for which in range(2):
        fetch(step, which).wait()
        for inner in range(width // 2):
            for slot in range(slots):
                for group in range(part // LANES):
                    held = (evens, odds)[(slot * (part // LANES) + group) % 2]
                    for row in range(LANES):
                        index = known[which][slot, inner * part + group * LANES + row]
                        held[pl.ds(row, 1), :] = wide[pl.ds(index + slot * rows, 1), :]
                    turned = held[...].T.astype(BF16)
                    out[
                        which * (width // 2) + inner,
                        :,
                        slot,
                        :,
                        group * LANES : (group + 1) * LANES,
                    ] = turned.reshape(out.shape[1], out.shape[3], LANES)

        @pl.when(step + 1 < steps)
        def _():
            fetch(step + 1, which).start()


def looked_up(ids, tables, place, sources, groups, share, offset, part):
    slots, rows, emb = tables.shape
    count = sources * slots * part
    width = 8
    layout = (share, groups * share, offset, part, width, sources)
    return pl.pallas_call(
        functools.partial(lookup_kernel, layout),
        grid_spec=pltpu.PrefetchScalarGridSpec(
            num_scalar_prefetch=1,
            grid=(sources // width,),
            in_specs=[
                pl.BlockSpec(memory_space=pltpu.HBM),
                pl.BlockSpec((slots, rows, emb), lambda i, place: (0, 0, 0)),
            ],
            out_specs=pl.BlockSpec(
                (width, groups, slots, emb // groups, part), lambda i, place: (i, 0, 0, 0, 0)
            ),
            scratch_shapes=[
                pltpu.VMEM((slots * rows, emb), F32),
                pltpu.VMEM((LANES, emb), F32),
                pltpu.VMEM((LANES, emb), F32),
                pltpu.VMEM((slots, sources * part), jnp.int32),
                pltpu.SMEM((slots, width // 2 * part), jnp.int32),
                pltpu.SMEM((slots, width // 2 * part), jnp.int32),
                pltpu.SemaphoreType.DMA((sources,)),
                pltpu.SemaphoreType.DMA((2,)),
            ],
        ),
        out_shape=jax.ShapeDtypeStruct((sources, groups, slots, emb // groups, part), BF16),
        cost_estimate=cost(count * 1_000_000, count * emb * 2),
        compiler_params=pltpu.CompilerParams(vmem_limit_bytes=VMEM),
        name="lookup",
    )(place, ids, tables)


def first_kernel(moved, placing, down, embedded, product, turned):
    _, many, _, emb, part = moved.shape
    wide = placing.shape[1]
    for inner in range(emb // SUBLANES):
        for group in range(many):
            for piece in range(part // LANES):
                block = moved[
                    :,
                    group,
                    :,
                    inner * SUBLANES : (inner + 1) * SUBLANES,
                    piece * LANES : (piece + 1) * LANES,
                ]
                at = (group * (part // LANES) + piece) * LANES
                turned[at : at + LANES, :] = (
                    block.astype(F32).reshape(wide, LANES).T.astype(BF16)
                )
        embedded[:, inner * wide : (inner + 1) * wide] = jnp.dot(
            turned[...], placing[...], preferred_element_type=F32
        ).astype(BF16)
    product[...] = jnp.dot(embedded[...], down[0], preferred_element_type=F32).astype(BF16)


def first(moved, placing, down, rows_each):
    sources, groups, slots, emb, part = moved.shape
    wide = placing.shape[0]
    width = sources * slots * emb
    rank = down.shape[2]
    rows = groups * part
    many = rows_each // part
    return pl.pallas_call(
        first_kernel,
        grid=(groups // many,),
        in_specs=[
            pl.BlockSpec((sources, many, slots, emb, part), lambda i: (0, i, 0, 0, 0)),
            pl.BlockSpec((wide, wide), lambda i: (0, 0)),
            pl.BlockSpec((1, width, rank), lambda i: (0, 0, 0)),
        ],
        out_specs=[
            pl.BlockSpec((rows_each, width), lambda i: (i, 0)),
            pl.BlockSpec((rows_each, rank), lambda i: (i, 0)),
        ],
        scratch_shapes=[pltpu.VMEM((rows_each, wide), BF16)],
        out_shape=[
            jax.ShapeDtypeStruct((rows, width), BF16),
            jax.ShapeDtypeStruct((rows, rank), BF16),
        ],
        cost_estimate=cost(4 * rows * width * rank, 4 * rows * width),
        compiler_params=pltpu.CompilerParams(vmem_limit_bytes=CROSS_VMEM),
        name="first",
    )(moved, placing, down)


def low_of(place, mine, near, far, across):
    own = pl.program_id(0) == place[0] % 2
    pair = (mine[...].astype(F32) + near[...].astype(F32)).astype(BF16).astype(F32)
    other = jnp.where(own, far[...].astype(F32), across[...].astype(F32))
    return (pair + other).astype(BF16)


def middle_kernel(place, mine, near, far, across, embedded, up, bias, down, state, product):
    low = low_of(place, mine, near, far, across)
    width = embedded.shape[1]
    tile = 512
    for at in range(0, width, tile):
        cut = slice(at, at + tile)
        high = jnp.dot(low, up[0, :, cut], preferred_element_type=F32) + bias[0:1, cut]
        own = embedded[:, cut].astype(F32)
        state[:, cut] = (own * high + own).astype(BF16)
    product[...] = jnp.dot(state[...], down[0], preferred_element_type=F32).astype(BF16)


def low_specs(half, rank):
    return [
        pl.BlockSpec((half, rank), lambda i, place: (i, 0)),
        pl.BlockSpec((half, rank), lambda i, place: (i, 0)),
        pl.BlockSpec((half, rank), lambda i, place: (0, 0)),
        pl.BlockSpec((half, rank), lambda i, place: (0, 0)),
    ]


def middle(place, lows, embedded, up, bias, down, layer):
    rows, width = embedded.shape
    rank = up.shape[1]
    half = rows // 2
    return pl.pallas_call(
        middle_kernel,
        grid_spec=pltpu.PrefetchScalarGridSpec(
            num_scalar_prefetch=1,
            grid=(2,),
            in_specs=low_specs(half, rank)
            + [
                pl.BlockSpec((half, width), lambda i, place: (i, 0)),
                pl.BlockSpec((1, rank, width), lambda i, place: (layer, 0, 0)),
                pl.BlockSpec((1, width), lambda i, place: (0, 0)),
                pl.BlockSpec((1, width, rank), lambda i, place: (layer + 1, 0, 0)),
            ],
            out_specs=[
                pl.BlockSpec((half, width), lambda i, place: (i, 0)),
                pl.BlockSpec((half, rank), lambda i, place: (i, 0)),
            ],
        ),
        out_shape=[
            jax.ShapeDtypeStruct((rows, width), BF16),
            jax.ShapeDtypeStruct((rows, rank), BF16),
        ],
        cost_estimate=cost(4 * rows * width * rank, 4 * rows * width),
        compiler_params=pltpu.CompilerParams(vmem_limit_bytes=CROSS_VMEM),
        name="middle",
    )(place, *lows, embedded, up, bias, down)


def last_kernel(place, mine, near, far, across, embedded, state, up, bias, *rest):
    out = rest[-1]
    low = low_of(place, mine, near, far, across)
    width = embedded.shape[1]
    groups, part = out.shape[0], out.shape[2]
    tile = 512
    for at in range(0, width, tile):
        cut = slice(at, at + tile)
        high = jnp.dot(low, up[0, :, cut], preferred_element_type=F32) + bias[0:1, cut]
        new = (
            embedded[:, cut].astype(F32) * high + state[:, cut].astype(F32)
        ).astype(BF16)
        out[:, 0, :, cut] = new.reshape(groups, part, tile)


def last(place, lows, embedded, state, up, bias, layer, so_far, groups, offset, part, share):
    rows, width = embedded.shape
    rank = up.shape[1]
    half = rows // 2
    in_specs = low_specs(half, rank) + [
        pl.BlockSpec((half, width), lambda i, place: (i, 0)),
        pl.BlockSpec((half, width), lambda i, place: (i, 0)),
        pl.BlockSpec((1, rank, width), lambda i, place: (layer, 0, 0)),
        pl.BlockSpec((1, width), lambda i, place: (0, 0)),
    ]
    args = [place, *lows, embedded, state, up, bias]
    aliases = {}
    if so_far is not None:
        in_specs.append(pl.BlockSpec(memory_space=pltpu.HBM))
        args.append(so_far)
        aliases = {9: 0}
    return pl.pallas_call(
        last_kernel,
        grid_spec=pltpu.PrefetchScalarGridSpec(
            num_scalar_prefetch=1,
            grid=(2,),
            in_specs=in_specs,
            out_specs=pl.BlockSpec(
                (groups // 2, 1, part, width), lambda i, place: (i, 0, offset // part, 0)
            ),
        ),
        out_shape=jax.ShapeDtypeStruct((groups, 1, share, width), BF16),
        input_output_aliases=aliases,
        cost_estimate=cost(2 * rows * width * rank, 6 * rows * width),
        compiler_params=pltpu.CompilerParams(vmem_limit_bytes=CROSS_VMEM),
        name="last",
    )(*args)


def summed(product):
    half = product.shape[0] // 2
    start = lax.rem(lax.axis_index("mp"), 2) * half
    near = lax.ppermute(product, "mp", CORE)
    pair = (
        lax.dynamic_slice_in_dim(product, start, half, 0).astype(F32)
        + lax.dynamic_slice_in_dim(near, start, half, 0).astype(F32)
    ).astype(BF16)
    far = lax.ppermute(pair, "mp", CHIP)
    across = lax.ppermute(far, "mp", CORE)
    return product, near, far, across


def per_device(lookup_ids, table_feature, tables, cross_down, cross_up, cross_bias):
    feats = table_feature.shape[0]
    sources = lax.axis_size("batch")
    groups = lax.axis_size("mp")
    total = lookup_ids.shape[1] // sources
    share = total // groups
    place = lax.axis_index("mp").reshape(1).astype(jnp.int32)
    same = table_feature[:, None] == jnp.arange(feats, dtype=jnp.int32)[None, :]
    row = jnp.arange(SUBLANES, dtype=jnp.int32)
    placing = (
        (same[:, None, None, :] & (row[:, None] == row[None, :])[None, :, :, None])
        .astype(BF16)
        .reshape(feats * SUBLANES, SUBLANES * feats)
    )
    out = None
    unit = share // sum(PIECES)
    parts = [piece * unit for piece in PIECES]
    offset = 0
    for part in parts:
        looked = looked_up(
            lookup_ids, tables, place, sources, groups, share, offset, part
        )
        shape = looked.shape
        moved = lax.all_to_all(
            looked.reshape(sources * groups, *shape[2:]),
            ("batch", "mp"),
            0,
            0,
            tiled=True,
        ).reshape(shape)
        embedded, product = first(moved, placing, cross_down, groups * part // 2)
        lows = summed(product)
        state, product = middle(place, lows, embedded, cross_up, cross_bias[:1], cross_down, 0)
        lows = summed(product)
        out = last(
            place,
            lows,
            embedded,
            state,
            cross_up,
            cross_bias[1:],
            1,
            out,
            groups,
            offset,
            part,
            share,
        )
        offset += part
    return out.reshape(total, -1)


def solution(mesh):
    return jax.shard_map(
        per_device,
        mesh=mesh,
        in_specs=(
            P("batch", None),
            P(),
            P("batch", None, None),
            P(None, "mp", None),
            P(None, None, "mp"),
            P(None, "mp"),
        ),
        out_specs=P("batch", "mp"),
        check_vma=False,
    )
```

```python
import functools

import jax
import jax.numpy as jnp
from jax import lax
from jax.experimental import pallas as pl
from jax.experimental.pallas import tpu as pltpu
from jax.sharding import PartitionSpec as P


LANES = 128
SUBLANES = 8
PIECES = (2, 2)
VMEM = 60 << 20
CROSS_VMEM = 24 << 20
CORE = [(0, 1), (1, 0), (2, 3), (3, 2)]
CHIP = [(0, 2), (2, 0), (1, 3), (3, 1)]
F32 = jnp.float32
BF16 = jnp.bfloat16


def cost(flops, moved):
    return pl.CostEstimate(flops=flops, bytes_accessed=moved, transcendentals=0)


def lookup_kernel(layout, place, ids, tables, out, wide, evens, odds, staged, *rest):
    share, stride, offset, part, width, sources = layout
    known, sems, moved, narrow, loaded = rest[:2], rest[2], rest[3], rest[4], rest[5]
    slots, rows, _ = tables.shape
    step = pl.program_id(0)
    steps = pl.num_programs(0)
    run = width // 2 * part
    tall = rows // 2

    def load(piece):
        slot, cut = piece // 2, pl.ds(piece % 2 * tall, tall)
        return pltpu.make_async_copy(
            tables.at[slot, cut, :], narrow.at[slot, cut, :], loaded.at[piece]
        )

    def stage(destination):
        start = destination * stride + place[0] * share + offset
        return pltpu.make_async_copy(
            ids.at[:, pl.ds(pl.multiple_of(start, LANES), part)],
            staged.at[:, pl.ds(destination * part, part)],
            sems.at[destination],
        )

    def fetch(at, which):
        start = (2 * at + which) * run
        return pltpu.make_async_copy(
            staged.at[:, pl.ds(pl.multiple_of(start, LANES), run)], known[which], moved.at[which]
        )

    @pl.when(step == 0)
    def _():
        for destination in range(sources):
            stage(destination).start()
        for piece in range(2 * slots):
            load(piece).start()
        for destination in range(sources):
            stage(destination).wait()
        for which in range(2):
            fetch(0, which).start()
        for piece in range(2 * slots):
            load(piece).wait()
            slot, first = piece // 2, piece % 2 * tall
            wide[pl.ds(piece * tall, tall), :] = narrow[slot, pl.ds(first, tall), :].astype(F32)

    for which in range(2):
        fetch(step, which).wait()
        for inner in range(width // 2):
            for slot in range(slots):
                for group in range(part // LANES):
                    held = (evens, odds)[(slot * (part // LANES) + group) % 2]
                    for row in range(LANES):
                        index = known[which][slot, inner * part + group * LANES + row]
                        held[pl.ds(row, 1), :] = wide[pl.ds(index + slot * rows, 1), :]
                    turned = held[...].T.astype(BF16)
                    out[
                        which * (width // 2) + inner,
                        :,
                        slot,
                        :,
                        group * LANES : (group + 1) * LANES,
                    ] = turned.reshape(out.shape[1], out.shape[3], LANES)

        @pl.when(step + 1 < steps)
        def _():
            fetch(step + 1, which).start()


def looked_up(ids, tables, place, sources, groups, share, offset, part):
    slots, rows, emb = tables.shape
    count = sources * slots * part
    width = 4
    layout = (share, groups * share, offset, part, width, sources)
    return pl.pallas_call(
        functools.partial(lookup_kernel, layout),
        grid_spec=pltpu.PrefetchScalarGridSpec(
            num_scalar_prefetch=1,
            grid=(sources // width,),
            in_specs=[
                pl.BlockSpec(memory_space=pltpu.HBM),
                pl.BlockSpec(memory_space=pltpu.HBM),
            ],
            out_specs=pl.BlockSpec(
                (width, groups, slots, emb // groups, part), lambda i, place: (i, 0, 0, 0, 0)
            ),
            scratch_shapes=[
                pltpu.VMEM((slots * rows, emb), F32),
                pltpu.VMEM((LANES, emb), F32),
                pltpu.VMEM((LANES, emb), F32),
                pltpu.VMEM((slots, sources * part), jnp.int32),
                pltpu.SMEM((slots, width // 2 * part), jnp.int32),
                pltpu.SMEM((slots, width // 2 * part), jnp.int32),
                pltpu.SemaphoreType.DMA((sources,)),
                pltpu.SemaphoreType.DMA((2,)),
                pltpu.VMEM((slots, rows, emb), BF16),
                pltpu.SemaphoreType.DMA((2 * slots,)),
            ],
        ),
        out_shape=jax.ShapeDtypeStruct((sources, groups, slots, emb // groups, part), BF16),
        cost_estimate=cost(count * 1_000_000, count * emb * 2),
        compiler_params=pltpu.CompilerParams(vmem_limit_bytes=VMEM),
        name="lookup",
    )(place, ids, tables)


def first_kernel(moved, placing, down, embedded, product, turned):
    _, many, _, emb, part = moved.shape
    wide = placing.shape[1]
    for inner in range(emb // SUBLANES):
        for group in range(many):
            for piece in range(part // LANES):
                block = moved[
                    :,
                    group,
                    :,
                    inner * SUBLANES : (inner + 1) * SUBLANES,
                    piece * LANES : (piece + 1) * LANES,
                ]
                at = (group * (part // LANES) + piece) * LANES
                turned[at : at + LANES, :] = (
                    block.astype(F32).reshape(wide, LANES).T.astype(BF16)
                )
        embedded[:, inner * wide : (inner + 1) * wide] = jnp.dot(
            turned[...], placing[...], preferred_element_type=F32
        ).astype(BF16)
    product[...] = jnp.dot(embedded[...], down[0], preferred_element_type=F32).astype(BF16)


def first(moved, placing, down, rows_each):
    sources, groups, slots, emb, part = moved.shape
    wide = placing.shape[0]
    width = sources * slots * emb
    rank = down.shape[2]
    rows = groups * part
    many = rows_each // part
    return pl.pallas_call(
        first_kernel,
        grid=(groups // many,),
        in_specs=[
            pl.BlockSpec((sources, many, slots, emb, part), lambda i: (0, i, 0, 0, 0)),
            pl.BlockSpec((wide, wide), lambda i: (0, 0)),
            pl.BlockSpec((1, width, rank), lambda i: (0, 0, 0)),
        ],
        out_specs=[
            pl.BlockSpec((rows_each, width), lambda i: (i, 0)),
            pl.BlockSpec((rows_each, rank), lambda i: (i, 0)),
        ],
        scratch_shapes=[pltpu.VMEM((rows_each, wide), BF16)],
        out_shape=[
            jax.ShapeDtypeStruct((rows, width), BF16),
            jax.ShapeDtypeStruct((rows, rank), BF16),
        ],
        cost_estimate=cost(4 * rows * width * rank, 4 * rows * width),
        compiler_params=pltpu.CompilerParams(vmem_limit_bytes=CROSS_VMEM),
        name="first",
    )(moved, placing, down)


def low_of(place, mine, near, far, across):
    own = pl.program_id(0) == place[0] % 2
    pair = (mine[...].astype(F32) + near[...].astype(F32)).astype(BF16).astype(F32)
    other = jnp.where(own, far[...].astype(F32), across[...].astype(F32))
    return (pair + other).astype(BF16)


def middle_kernel(place, mine, near, far, across, embedded, up, bias, down, state, product):
    low = low_of(place, mine, near, far, across)
    width = embedded.shape[1]
    tile = 512
    for at in range(0, width, tile):
        cut = slice(at, at + tile)
        high = jnp.dot(low, up[0, :, cut], preferred_element_type=F32) + bias[0:1, cut]
        own = embedded[:, cut].astype(F32)
        state[:, cut] = (own * high + own).astype(BF16)
    product[...] = jnp.dot(state[...], down[0], preferred_element_type=F32).astype(BF16)


def low_specs(half, rank):
    return [
        pl.BlockSpec((half, rank), lambda i, place: (i, 0)),
        pl.BlockSpec((half, rank), lambda i, place: (i, 0)),
        pl.BlockSpec((half, rank), lambda i, place: (0, 0)),
        pl.BlockSpec((half, rank), lambda i, place: (0, 0)),
    ]


def middle(place, lows, embedded, up, bias, down, layer):
    rows, width = embedded.shape
    rank = up.shape[1]
    half = rows // 2
    return pl.pallas_call(
        middle_kernel,
        grid_spec=pltpu.PrefetchScalarGridSpec(
            num_scalar_prefetch=1,
            grid=(2,),
            in_specs=low_specs(half, rank)
            + [
                pl.BlockSpec((half, width), lambda i, place: (i, 0)),
                pl.BlockSpec((1, rank, width), lambda i, place: (layer, 0, 0)),
                pl.BlockSpec((1, width), lambda i, place: (0, 0)),
                pl.BlockSpec((1, width, rank), lambda i, place: (layer + 1, 0, 0)),
            ],
            out_specs=[
                pl.BlockSpec((half, width), lambda i, place: (i, 0)),
                pl.BlockSpec((half, rank), lambda i, place: (i, 0)),
            ],
        ),
        out_shape=[
            jax.ShapeDtypeStruct((rows, width), BF16),
            jax.ShapeDtypeStruct((rows, rank), BF16),
        ],
        cost_estimate=cost(4 * rows * width * rank, 4 * rows * width),
        compiler_params=pltpu.CompilerParams(vmem_limit_bytes=CROSS_VMEM),
        name="middle",
    )(place, *lows, embedded, up, bias, down)


def last_kernel(place, mine, near, far, across, embedded, state, up, bias, *rest):
    out = rest[-1]
    low = low_of(place, mine, near, far, across)
    width = embedded.shape[1]
    groups, part = out.shape[0], out.shape[2]
    tile = 512
    for at in range(0, width, tile):
        cut = slice(at, at + tile)
        high = jnp.dot(low, up[0, :, cut], preferred_element_type=F32) + bias[0:1, cut]
        new = (
            embedded[:, cut].astype(F32) * high + state[:, cut].astype(F32)
        ).astype(BF16)
        out[:, 0, :, cut] = new.reshape(groups, part, tile)


def last(place, lows, embedded, state, up, bias, layer, so_far, groups, offset, part, share):
    rows, width = embedded.shape
    rank = up.shape[1]
    half = rows // 2
    in_specs = low_specs(half, rank) + [
        pl.BlockSpec((half, width), lambda i, place: (i, 0)),
        pl.BlockSpec((half, width), lambda i, place: (i, 0)),
        pl.BlockSpec((1, rank, width), lambda i, place: (layer, 0, 0)),
        pl.BlockSpec((1, width), lambda i, place: (0, 0)),
    ]
    args = [place, *lows, embedded, state, up, bias]
    aliases = {}
    if so_far is not None:
        in_specs.append(pl.BlockSpec(memory_space=pltpu.HBM))
        args.append(so_far)
        aliases = {9: 0}
    return pl.pallas_call(
        last_kernel,
        grid_spec=pltpu.PrefetchScalarGridSpec(
            num_scalar_prefetch=1,
            grid=(2,),
            in_specs=in_specs,
            out_specs=pl.BlockSpec(
                (groups // 2, 1, part, width), lambda i, place: (i, 0, offset // part, 0)
            ),
        ),
        out_shape=jax.ShapeDtypeStruct((groups, 1, share, width), BF16),
        input_output_aliases=aliases,
        cost_estimate=cost(2 * rows * width * rank, 6 * rows * width),
        compiler_params=pltpu.CompilerParams(vmem_limit_bytes=CROSS_VMEM),
        name="last",
    )(*args)


def summed(product):
    half = product.shape[0] // 2
    start = lax.rem(lax.axis_index("mp"), 2) * half
    near = lax.ppermute(product, "mp", CORE)
    pair = (
        lax.dynamic_slice_in_dim(product, start, half, 0).astype(F32)
        + lax.dynamic_slice_in_dim(near, start, half, 0).astype(F32)
    ).astype(BF16)
    far = lax.ppermute(pair, "mp", CHIP)
    across = lax.ppermute(far, "mp", CORE)
    return product, near, far, across


def per_device(lookup_ids, table_feature, tables, cross_down, cross_up, cross_bias):
    feats = table_feature.shape[0]
    sources = lax.axis_size("batch")
    groups = lax.axis_size("mp")
    total = lookup_ids.shape[1] // sources
    share = total // groups
    place = lax.axis_index("mp").reshape(1).astype(jnp.int32)
    same = table_feature[:, None] == jnp.arange(feats, dtype=jnp.int32)[None, :]
    row = jnp.arange(SUBLANES, dtype=jnp.int32)
    placing = (
        (same[:, None, None, :] & (row[:, None] == row[None, :])[None, :, :, None])
        .astype(BF16)
        .reshape(feats * SUBLANES, SUBLANES * feats)
    )
    out = None
    unit = share // sum(PIECES)
    parts = [piece * unit for piece in PIECES]
    offset = 0
    for part in parts:
        looked = looked_up(
            lookup_ids, tables, place, sources, groups, share, offset, part
        )
        shape = looked.shape
        moved = lax.all_to_all(
            looked.reshape(sources * groups, *shape[2:]),
            ("batch", "mp"),
            0,
            0,
            tiled=True,
        ).reshape(shape)
        embedded, product = first(moved, placing, cross_down, groups * part // 2)
        lows = summed(product)
        state, product = middle(place, lows, embedded, cross_up, cross_bias[:1], cross_down, 0)
        lows = summed(product)
        out = last(
            place,
            lows,
            embedded,
            state,
            cross_up,
            cross_bias[1:],
            1,
            out,
            groups,
            offset,
            part,
            share,
        )
        offset += part
    return out.reshape(total, -1)


def solution(mesh):
    return jax.shard_map(
        per_device,
        mesh=mesh,
        in_specs=(
            P("batch", None),
            P(),
            P("batch", None, None),
            P(None, "mp", None),
            P(None, None, "mp"),
            P(None, "mp"),
        ),
        out_specs=P("batch", "mp"),
        check_vma=False,
    )
```
